256 devices in a mesh: blk: 64 (over y, z, core), plane: 4 (over x).
Axes of the slice: x: 4, y: 4, z: 8, core: 2. Of those that a mesh axis runs over, the one named last changes fastest.
Arguments:
- tiles: bfloat16 [1024, 24, 128, 128], P(('blk', 'plane')), may hold values from -0.078125 to 0.078125
- tile_cols: int32 [1024, 24], P(('blk', 'plane')), may hold values from 0 to 511
- tile_count: int32 [1024], P(('blk', 'plane')), may hold values from 18 to 24, as said below
- u_start: float32 [131072], P(('blk', 'plane')), may hold values from -0.015625 to 0.015625
- v_start: float32 [65536], P(('blk', 'plane')), may hold values from -0.0234375 to 0.0234375
- beta_start: float32 [1], replicated, may hold values from 0.5 to 1.5
- left_basis: float32 [131072, 128], P(('blk', 'plane')), may hold values from -0.015625 to 0.015625
- right_basis: float32 [65536, 128], P(('blk', 'plane')), may hold values from -0.0234375 to 0.0234375
Outputs:
- left_vectors: float32 [1, 131072], P(None, ('blk', 'plane'))
- right_vectors: float32 [1, 65536], P(None, ('blk', 'plane'))
- coefficients: float32 [2], replicated
The draws below stay inside these ranges and needn't reach their ends.
Inputs may be any that keep to these rules, and one draw needn't show every extreme that they name: `tile_count`: slots at and after a row block's count are padding; some row block uses all 24 slots.
All inputs are finite; a program needn't handle non-finite values.
Results may differ from the reference program's by a relative error of at most 0.00055.
The reference program's roundings to bfloat16 on the way count: a program that leaves them out, or rounds other values in their place, can miss the bound.
Values may be sent and summed in bfloat16 or wider, within the bound.
A program may use at most 64 MiB of HBM per device.

```python
import jax
import jax.numpy as jnp
from jax import lax

N = 65536
NT = 512
SLOTS = 24
KB = 128
ITERS = 1
BLOCKS = 1024
ROWS = 131072


def draw_tile_count(key, part):
    counts = jax.random.randint(key, (BLOCKS,), max(1, 3 * SLOTS // 4), SLOTS + 1).astype(jnp.int32)
    return counts.at[0].set(SLOTS)


def plant(drawn, own_key, smallest, top_value):
    dims = drawn.shape
    spot = [jax.random.randint(jax.random.fold_in(own_key, axis), (), 0, dims[axis]) for axis in range(len(dims))]
    drawn = drawn.at[tuple(spot)].set(smallest)
    longest = dims.index(max(dims))
    spot[longest] = (spot[longest] + 1) % dims[longest]
    return drawn.at[tuple(spot)].set(top_value)


def block_scale(stream_key, extent, cuts, low, largest):
    level, own = 1.0, jax.random.fold_in(stream_key, 6)
    for position, shards_of in cuts:
        draws = jnp.exp(jax.random.uniform(jax.random.fold_in(own, position), (shards_of,), jnp.float32, low / len(cuts), largest / len(cuts)))
        level = level * jnp.repeat(draws, extent[position] // shards_of).reshape([-1 if axis == position else 1 for axis in range(len(extent))])
    return level


def centred(rng, shape, spread, limit, shards=(), kind=jnp.bfloat16):
    drawn = spread * jax.random.normal(rng, shape, jnp.float32)
    if shards:
        drawn = drawn * block_scale(rng, shape, shards, -0.22, 0.18)
    return jnp.clip(drawn, -limit, limit).astype(kind)


def setup_inputs(seed: int = 0) -> dict:
    key_of = jax.random.split(jax.random.key(seed), 9)
    tiles = centred(key_of[0], (BLOCKS, SLOTS, 128, 128), (ROWS * SLOTS * 112 // N) ** -0.5, 0.078125, ((0, 256),))
    tile_cols = plant(jax.random.randint(key_of[1], (BLOCKS, SLOTS), 0, NT), jax.random.fold_in(key_of[1], 1), 0, NT - 1).astype(jnp.int32)
    tile_count = draw_tile_count(jax.random.fold_in(key_of[8], 71), 0)
    u_start = centred(key_of[3], (ROWS,), ROWS ** -0.5, 0.015625, ((0, 256),), jnp.float32)
    v_start = centred(key_of[4], (N,), N ** -0.5, 0.0234375, ((0, 256),), jnp.float32)
    beta_start = jnp.clip(jax.random.uniform(key_of[5], (1,), jnp.float32, 0.5, 1.5), 0.5, 1.5)
    left_basis = centred(key_of[6], (ROWS, KB), ROWS ** -0.5, 0.015625, ((0, 256),), jnp.float32)
    right_basis = centred(key_of[7], (N, KB), N ** -0.5, 0.0234375, ((0, 256),), jnp.float32)
    return dict(tiles=tiles, tile_cols=tile_cols, tile_count=tile_count, u_start=u_start, v_start=v_start, beta_start=beta_start, left_basis=left_basis, right_basis=right_basis)


def project_twice(vec, basis):
    high = lax.Precision.HIGHEST
    first = jnp.dot(vec, basis, precision=high)
    vec = vec - jnp.dot(basis, first, precision=high)
    second = jnp.dot(vec, basis, precision=high)
    vec = vec - jnp.dot(basis, second, precision=high)
    norm = jnp.sqrt(jnp.sum(vec * vec) + 1e-06)
    return (vec / norm, norm)

def reference(tiles, tile_cols, tile_count, u_start, v_start, beta_start, left_basis, right_basis):
    high = lax.Precision.HIGHEST
    live = (jnp.arange(SLOTS, dtype=jnp.int32)[None, :] < tile_count[:, None]).astype(jnp.float32)

    def forward(rounded):
        table = rounded.reshape(-1, 128)

        def single(items):
            block, cols, weight = items
            picked = table[cols].astype(jnp.float32)
            values = jnp.einsum('sij,sj->si', block.astype(jnp.float32), picked, precision=high)
            return lax.optimization_barrier(jnp.sum(values * weight[:, None], axis=0))
        return lax.map(single, (tiles, tile_cols, live)).reshape(-1)

    def backward(rounded):
        table = rounded.reshape(-1, 128)

        def single(items):
            block, row, weight = items
            values = jnp.einsum('sij,i->sj', block.astype(jnp.float32), row.astype(jnp.float32), precision=high)
            return values * weight[:, None]
        contrib = lax.map(single, (tiles, table, live)).reshape(-1, 128)
        summed = jax.ops.segment_sum(contrib, tile_cols.reshape(-1), num_segments=N // 128)
        return summed.reshape(-1)
    vec_right = v_start
    vec_left = u_start
    beta = beta_start[0]
    lefts, rights, coefs = ([], [], [])
    for step in range(ITERS):
        forward_out = forward(vec_right.astype(jnp.bfloat16))
        vec_left, alpha = project_twice(forward_out - beta * vec_left, left_basis)
        back_out = backward(vec_left.astype(jnp.bfloat16))
        vec_right, beta = project_twice(back_out - alpha * vec_right, right_basis)
        lefts.append(vec_left * jnp.sqrt(jnp.float32(ROWS)))
        rights.append(vec_right * jnp.sqrt(jnp.float32(N)))
        coefs.append(alpha)
        coefs.append(beta)
    return (jnp.stack(lefts), jnp.stack(rights), jnp.stack(coefs))
```

```python
import math

import jax
import jax.numpy as jnp
from jax import lax
from jax.experimental import pallas as pl
from jax.experimental.pallas import tpu as pltpu
from jax.sharding import PartitionSpec as P

MESH = pl.DeviceIdType.MESH
HIGH = lax.Precision.HIGHEST
F32 = jnp.float32
BF16 = jnp.bfloat16

X, Y, Z, C = 4, 4, 8, 2
PLANE = X * Y * C
BLOCKS = 4
SLOTS = 24
LANES = 32

AG_Z, AG_P, G_P, G_Z, G_ALL, C_P, C_Z, S_P, S_Z, D_P, D_Z = range(11)
EXCHANGES = 11


def high_dot(a, b):
    return jnp.dot(a, b, precision=HIGH, preferred_element_type=F32)


def gram(basis):
    return lax.dot_general(
        basis, basis, (((0,), (0,)), ((), ())), precision=HIGH, preferred_element_type=F32
    )


def kernel(
    left_scale,
    right_scale,
    tiles_h,
    cols_h,
    cnt_h,
    u_h,
    v_h,
    beta_h,
    lb_h,
    rb_h,
    out_ref,
    tiles,
    cols,
    cnt,
    beta,
    u_in,
    v_in,
    lb,
    rb,
    rowid,
    onehot,
    vz,
    vtab,
    table,
    acc_ref,
    gsend,
    g_p,
    gz_send,
    g_z,
    gp_send,
    g_all,
    ml,
    nl,
    mr,
    nr,
    c_send,
    c_p,
    cz_send,
    c_z,
    contrib,
    ub_ref,
    u_ref,
    s_send,
    s_p,
    sz_send,
    s_z,
    d_send,
    d_p,
    dz_send,
    d_z,
    local_sem,
    send_sem,
    recv_sem,
):
    blk = lax.axis_index("blk")
    x = lax.axis_index("plane")
    core = lax.rem(blk, C)
    z = lax.rem(lax.div(blk, C), Z)
    y = lax.div(blk, C * Z)
    g = y * (C * X) + core * X + x

    loads = [
        pltpu.make_async_copy(a, b, local_sem.at[i])
        for i, (a, b) in enumerate(
            [
                (v_h, v_in),
                (cols_h, cols),
                (cnt_h, cnt),
                (u_h, u_in),
                (beta_h, beta),
                (lb_h, lb),
                (rb_h, rb),
            ]
            + [(tiles_h.at[r], tiles.at[r]) for r in range(BLOCKS)]
        )
    ]
    for copy in loads:
        copy.start()

    xs = [lax.rem(x + d, X) for d in range(X)]
    ys = [lax.rem(y + d, Y) for d in range(Y)]
    cs = [lax.rem(core + d, C) for d in range(C)]
    zs = [lax.rem(z + d, Z) for d in range(Z)]
    far_x = sorted(range(X), key=lambda d: -min(d, X - d))
    far_y = sorted(range(Y), key=lambda d: -min(d, Y - d))
    plane_offsets = sorted(
        [(dx, dy, dc) for dx in far_x for dy in far_y for dc in (1, 0) if (dx, dy, dc) != (0, 0, 0)],
        key=lambda o: -(min(o[0], X - o[0]) + min(o[1], Y - o[1])),
    )
    z_offsets = sorted(range(1, Z), key=lambda d: -min(d, Z - d))

    def plane_peers():
        for dx, dy, dc in plane_offsets:
            yield (
                (ys[dy] * (Z * C) + z * C + cs[dc], xs[dx]),
                ys[dy] * (C * X) + cs[dc] * X + xs[dx],
            )

    def z_peers():
        for d in z_offsets:
            yield (y * (Z * C) + zs[d] * C + core, x), zs[d]

    def send(which, src, dst, device):
        pltpu.make_async_remote_copy(
            src_ref=src,
            dst_ref=dst,
            send_sem=send_sem.at[which],
            recv_sem=recv_sem.at[which],
            device_id=device,
            device_id_type=MESH,
        ).start()

    def arrived(which, slots, count):
        part = slots.at[pl.ds(0, count)]
        pltpu.make_async_copy(part, part, recv_sem.at[which]).wait()

    def sent(which, slots, count):
        part = slots.at[pl.ds(0, count)]
        pltpu.make_async_copy(part, part, send_sem.at[which]).wait()

    barrier = pltpu.get_barrier_semaphore()
    for device, _ in z_peers():
        pl.semaphore_signal(barrier, inc=1, device_id=device, device_id_type=MESH)
    for device, _ in plane_peers():
        pl.semaphore_signal(barrier, inc=1, device_id=device, device_id_type=MESH)

    eye = lax.broadcasted_iota(jnp.int32, (128, 128), 0) == lax.broadcasted_iota(
        jnp.int32, (128, 128), 1
    )
    diagonal = jnp.where(eye, 1.0, 0.0).astype(F32)
    for copy in loads[:7]:
        copy.wait()

    lane = lax.broadcasted_iota(jnp.int32, (1, 128), 1)
    at = jnp.full((1, 128), -1, jnp.int32)
    for r in range(BLOCKS):
        for s in range(SLOTS):
            t = cols[r, s]
            row = (t & 0x181) | ((t & 0xE) << 3) | ((t & 0x70) >> 3)
            row = jnp.where(s < cnt[r], row, PLANE * Z * 2)
            rowid[r * SLOTS + s] = row
            at = jnp.where(lane == r * LANES + s, row, at)
    onehot[...] = jnp.where(
        lax.broadcasted_iota(jnp.int32, (PLANE * Z * 2, 128), 0) == at, 1.0, 0.0
    ).astype(BF16)
    table[pl.ds(PLANE * Z * 2, 8), :] = jnp.zeros((8, 128), F32)
    contrib[...] = jnp.zeros_like(contrib)
    beta_u = u_in[...] * beta[0]
    for r in range(BLOCKS):
        acc_ref[r] = jnp.where(eye, -beta_u[r : r + 1, :], 0.0)
    vz[z] = v_in[...]
    gsend[:, 0:4, :] = gram(lb[...]).reshape(PLANE, 4, 128)
    gsend[:, 4:8, :] = gram(rb[...]).reshape(PLANE, 4, 128)

    pl.semaphore_wait(barrier, PLANE - 1 + Z - 1)

    for device, _ in z_peers():
        send(AG_Z, v_in, vz.at[z], device)
    for device, peer in plane_peers():
        send(G_P, gsend.at[peer], g_p.at[g], device)
    g_p[g] = gsend[g]
    arrived(AG_Z, vz, Z - 1)
    vtab[g] = vz[...].reshape(2 * Z, 128).astype(BF16)
    for device, _ in plane_peers():
        send(AG_P, vtab.at[g], vtab.at[g], device)
    arrived(G_P, g_p, PLANE - 1)
    gz = jnp.sum(g_p[...], axis=0)
    gz_send[...] = gz
    g_z[z] = gz
    for device, _ in z_peers():
        send(G_Z, gz_send, g_z.at[z], device)
    for copy in loads[7:]:
        copy.wait()
    arrived(AG_P, vtab, PLANE - 1)
    table[pl.ds(0, PLANE * Z * 2), :] = vtab[...].astype(F32).reshape(PLANE * Z * 2, 128)

    ps = []
    for r in range(BLOCKS):

        def forward(s, acc, r=r):
            row = table[pl.ds(rowid[r * SLOTS + s], 1), :]
            return acc + tiles[r, s].astype(F32) * row

        acc = lax.fori_loop(0, SLOTS, forward, acc_ref[r], unroll=4)
        ps.append(jnp.broadcast_to(jnp.sum(acc, axis=1, keepdims=True), (128, 128)))

    def inner(basis_rows, columns):
        first = sum(
            jnp.sum(b * c, axis=0, keepdims=True) for b, c in zip(basis_rows, columns)
        )
        square = sum(jnp.sum(c * c, axis=0, keepdims=True) for c in columns)
        return first, square

    def total(slots):
        return jnp.sum(slots[...], axis=0)

    first, square = inner([lb[pl.ds(r * 128, 128), :] for r in range(BLOCKS)], ps)
    c_send[0:1, :] = first
    c_send[1:2, :] = square
    c_p[g] = c_send[...]
    for device, _ in plane_peers():
        send(C_P, c_send, c_p.at[g], device)
    for r in range(BLOCKS):
        acc_ref[r] = ps[r]
    arrived(G_Z, g_z, Z - 1)
    gp = jnp.sum(g_z[...], axis=0)
    gp_send[...] = gp
    g_all[g] = gp
    for device, _ in plane_peers():
        send(G_ALL, gp_send, g_all.at[g], device)
    arrived(C_P, c_p, PLANE - 1)
    cz = total(c_p)
    cz_send[...] = cz
    c_z[z] = cz
    for device, _ in z_peers():
        send(C_Z, cz_send, c_z.at[z], device)
    arrived(G_ALL, g_all, PLANE - 1)
    left_gram = g_all[:, 0:4, :].reshape(128, 128)
    right_gram = g_all[:, 4:8, :].reshape(128, 128)

    def twice(gram_matrix):
        b = 2.0 * diagonal - gram_matrix
        return b, 2.0 * b - high_dot(b, high_dot(gram_matrix, b))

    bl, nl[...] = twice(left_gram)
    ml[...] = high_dot(lb[...], bl)

    def norm_of(first, square, quadratic):
        column = jnp.sum(quadratic * first, axis=1, keepdims=True)
        inner_sum = jnp.sum(jnp.where(eye, column, 0.0) * first, axis=0, keepdims=True)
        inner_sum = jnp.sum(inner_sum, axis=1, keepdims=True)
        return jnp.sqrt(square - inner_sum + 1e-6)

    arrived(C_Z, c_z, Z - 1)
    both = total(c_z)
    first, square = both[0:1, :], both[1:2, :]
    alpha = norm_of(first, square, nl[...])
    contribs = []
    for r in range(BLOCKS):
        less = jnp.sum(ml[pl.ds(r * 128, 128), :] * first, axis=1, keepdims=True)
        u = (acc_ref[r] - less) / alpha
        u_ref[r] = u
        ub_ref[r] = u.astype(BF16).astype(F32)
    for r in range(BLOCKS):

        def backward(s, _, r=r):
            part = jnp.sum(tiles[r, s].astype(F32) * ub_ref[r], axis=0, keepdims=True)
            contrib[pl.ds(r * LANES + s, 1), :] = part
            return 0

        lax.fori_loop(0, SLOTS, backward, 0, unroll=4)
    whole = contrib[...]
    high = whole.astype(BF16)
    rest = whole - high.astype(F32)
    middle = rest.astype(BF16)
    low = (rest - middle.astype(F32)).astype(BF16)
    hot = onehot[...]
    partial = (
        jnp.dot(hot, high, preferred_element_type=F32)
        + jnp.dot(hot, middle, preferred_element_type=F32)
        + jnp.dot(hot, low, preferred_element_type=F32)
    )
    s_send[...] = partial.reshape(PLANE, 2 * Z, 128)
    for device, peer in plane_peers():
        send(S_P, s_send.at[peer], s_p.at[g], device)
    s_p[g] = s_send[g]
    for r in range(BLOCKS):
        out_ref[r : r + 1, :] = left_scale * jnp.sum(
            jnp.where(eye, u_ref[r], 0.0), axis=0, keepdims=True
        )
    br, nr[...] = twice(right_gram)
    mr[...] = high_dot(rb[...], br)
    arrived(S_P, s_p, PLANE - 1)
    sz_send[...] = total(s_p).reshape(Z, 2, 128)
    s_z[z] = sz_send[z]
    for device, peer in z_peers():
        send(S_Z, sz_send.at[peer], s_z.at[z], device)
    arrived(S_Z, s_z, Z - 1)
    residual = total(s_z) - alpha * v_in[...]
    rs = [
        jnp.broadcast_to(
            jnp.sum(jnp.where(eye, residual[h : h + 1, :], 0.0), axis=1, keepdims=True), (128, 128)
        )
        for h in range(2)
    ]
    first, square = inner([rb[pl.ds(h * 128, 128), :] for h in range(2)], rs)
    d_send[0:1, :] = first
    d_send[1:2, :] = square
    d_p[g] = d_send[...]
    for device, _ in plane_peers():
        send(D_P, d_send, d_p.at[g], device)
    arrived(D_P, d_p, PLANE - 1)
    dz = total(d_p)
    dz_send[...] = dz
    d_z[z] = dz
    for device, _ in z_peers():
        send(D_Z, dz_send, d_z.at[z], device)
    arrived(D_Z, d_z, Z - 1)
    both = total(d_z)
    first, square = both[0:1, :], both[1:2, :]
    new_beta = norm_of(first, square, nr[...])
    for h in range(2):
        less = jnp.sum(mr[pl.ds(h * 128, 128), :] * first, axis=1, keepdims=True)
        v = (rs[h] - less) / new_beta
        out_ref[4 + h : 5 + h, :] = right_scale * jnp.sum(
            jnp.where(eye, v, 0.0), axis=0, keepdims=True
        )
    out_ref[6:7, :] = jnp.where(lane == 0, alpha, new_beta)
    out_ref[7:8, :] = jnp.zeros((1, 128), F32)

    for which, slots, count in (
        (AG_Z, vz, Z - 1),
        (AG_P, vtab, PLANE - 1),
        (G_P, g_p, PLANE - 1),
        (G_Z, g_z, Z - 1),
        (G_ALL, g_all, PLANE - 1),
        (C_P, c_p, PLANE - 1),
        (C_Z, c_z, Z - 1),
        (S_P, s_p, PLANE - 1),
        (S_Z, s_z, Z - 1),
        (D_P, d_p, PLANE - 1),
        (D_Z, d_z, Z - 1),
    ):
        sent(which, slots, count)


def solution(mesh):
    devices = math.prod(mesh.shape.values())

    def step(tiles, tile_cols, tile_count, u_start, v_start, beta_start, left_basis, right_basis):
        vmem = pltpu.VMEM
        out = pl.pallas_call(
            lambda *refs: kernel(
                math.sqrt(u_start.shape[0] * devices), math.sqrt(v_start.shape[0] * devices), *refs
            ),
            name="lanczos_step",
            out_shape=jax.ShapeDtypeStruct((8, 128), F32),
            in_specs=[pl.BlockSpec(memory_space=pl.ANY)] * 8,
            out_specs=pl.BlockSpec(memory_space=pltpu.VMEM),
            scratch_shapes=[
                vmem((BLOCKS, SLOTS, 128, 128), BF16),
                pltpu.SMEM((BLOCKS, SLOTS), jnp.int32),
                pltpu.SMEM((BLOCKS,), jnp.int32),
                pltpu.SMEM((1,), F32),
                vmem((BLOCKS, 128), F32),
                vmem((2, 128), F32),
                vmem((BLOCKS * 128, 128), F32),
                vmem((2 * 128, 128), F32),
                pltpu.SMEM((BLOCKS * SLOTS,), jnp.int32),
                vmem((PLANE * Z * 2, 128), BF16),
                vmem((Z, 2, 128), F32),
                vmem((PLANE, 2 * Z, 128), BF16),
                vmem((PLANE * Z * 2 + 8, 128), F32),
                vmem((BLOCKS, 128, 128), F32),
                vmem((PLANE, 8, 128), F32),
                vmem((PLANE, 8, 128), F32),
                vmem((8, 128), F32),
                vmem((Z, 8, 128), F32),
                vmem((8, 128), F32),
                vmem((PLANE, 8, 128), F32),
                vmem((BLOCKS * 128, 128), F32),
                vmem((128, 128), F32),
                vmem((2 * 128, 128), F32),
                vmem((128, 128), F32),
                vmem((2, 128), F32),
                vmem((PLANE, 2, 128), F32),
                vmem((2, 128), F32),
                vmem((Z, 2, 128), F32),
                vmem((128, 128), F32),
                vmem((BLOCKS, 128, 128), F32),
                vmem((BLOCKS, 128, 128), F32),
                vmem((PLANE, 2 * Z, 128), F32),
                vmem((PLANE, 2 * Z, 128), F32),
                vmem((Z, 2, 128), F32),
                vmem((Z, 2, 128), F32),
                vmem((2, 128), F32),
                vmem((PLANE, 2, 128), F32),
                vmem((2, 128), F32),
                vmem((Z, 2, 128), F32),
                pltpu.SemaphoreType.DMA((7 + BLOCKS,)),
                pltpu.SemaphoreType.DMA((EXCHANGES,)),
                pltpu.SemaphoreType.DMA((EXCHANGES,)),
            ],
            compiler_params=pltpu.CompilerParams(collective_id=0, has_side_effects=True),
        )(
            tiles,
            tile_cols,
            tile_count,
            u_start.reshape(BLOCKS, 128),
            v_start.reshape(2, 128),
            beta_start,
            left_basis,
            right_basis,
        )
        return out[0:4].reshape(1, -1), out[4:6].reshape(1, -1), out[6, 0:2]

    both = ("blk", "plane")
    return jax.shard_map(
        step,
        mesh=mesh,
        in_specs=(
            P(both, None, None, None),
            P(both, None),
            P(both),
            P(both),
            P(both),
            P(),
            P(both, None),
            P(both, None),
        ),
        out_specs=(P(None, both), P(None, both), P()),
        check_vma=False,
    )
```

```python
import math

import jax
import jax.numpy as jnp
from jax import lax
from jax.experimental import pallas as pl
from jax.experimental.pallas import tpu as pltpu
from jax.sharding import PartitionSpec as P

MESH = pl.DeviceIdType.MESH
HIGH = lax.Precision.HIGHEST
F32 = jnp.float32
BF16 = jnp.bfloat16

X, Y, Z, C = 4, 4, 8, 2
PLANE = X * Y * C
BLOCKS = 4
SLOTS = 24
LANES = 32

AG_Z, AG_P, G_P, G_Z, G_ALL, C_P, C_Z, S_P, S_Z, D_P, D_Z = range(11)
EXCHANGES = 11


def high_dot(a, b):
    return jnp.dot(a, b, precision=HIGH, preferred_element_type=F32)


def gram(basis):
    return lax.dot_general(
        basis, basis, (((0,), (0,)), ((), ())), precision=HIGH, preferred_element_type=F32
    )


def kernel(
    left_scale,
    right_scale,
    tiles_h,
    cols_h,
    cnt_h,
    u_h,
    v_h,
    beta_h,
    lb_h,
    rb_h,
    out_ref,
    tiles,
    cols,
    cnt,
    beta,
    u_in,
    v_in,
    lb,
    rb,
    rowid,
    onehot,
    vz,
    vtab,
    table,
    acc_ref,
    gsend,
    g_p,
    gz_send,
    g_z,
    gp_send,
    g_all,
    ml,
    nl,
    mr,
    nr,
    c_send,
    c_p,
    cz_send,
    c_z,
    contrib,
    ub_ref,
    u_ref,
    s_send,
    s_p,
    sz_send,
    s_z,
    d_send,
    d_p,
    dz_send,
    d_z,
    local_sem,
    send_sem,
    recv_sem,
):
    blk = lax.axis_index("blk")
    x = lax.axis_index("plane")
    core = lax.rem(blk, C)
    z = lax.rem(lax.div(blk, C), Z)
    y = lax.div(blk, C * Z)
    g = y * (C * X) + core * X + x

    loads = [
        pltpu.make_async_copy(a, b, local_sem.at[i])
        for i, (a, b) in enumerate(
            [
                (v_h, v_in),
                (cols_h, cols),
                (cnt_h, cnt),
                (u_h, u_in),
                (beta_h, beta),
                (lb_h, lb),
                (rb_h, rb),
            ]
            + [(tiles_h.at[r], tiles.at[r]) for r in range(BLOCKS)]
        )
    ]
    for copy in loads:
        copy.start()

    xs = [lax.rem(x + d, X) for d in range(X)]
    ys = [lax.rem(y + d, Y) for d in range(Y)]
    cs = [lax.rem(core + d, C) for d in range(C)]
    zs = [lax.rem(z + d, Z) for d in range(Z)]
    far_x = sorted(range(X), key=lambda d: -min(d, X - d))
    far_y = sorted(range(Y), key=lambda d: -min(d, Y - d))
    plane_offsets = sorted(
        [(dx, dy, dc) for dx in far_x for dy in far_y for dc in (1, 0) if (dx, dy, dc) != (0, 0, 0)],
        key=lambda o: -(min(o[0], X - o[0]) + min(o[1], Y - o[1])),
    )
    z_offsets = sorted(range(1, Z), key=lambda d: -min(d, Z - d))

    def plane_peers():
        for dx, dy, dc in plane_offsets:
            yield (
                (ys[dy] * (Z * C) + z * C + cs[dc], xs[dx]),
                ys[dy] * (C * X) + cs[dc] * X + xs[dx],
            )

    def z_peers():
        for d in z_offsets:
            yield (y * (Z * C) + zs[d] * C + core, x), zs[d]

    def send(which, src, dst, device):
        pltpu.make_async_remote_copy(
            src_ref=src,
            dst_ref=dst,
            send_sem=send_sem.at[which],
            recv_sem=recv_sem.at[which],
            device_id=device,
            device_id_type=MESH,
        ).start()

    def arrived(which, slots, count):
        part = slots.at[pl.ds(0, count)]
        with jax.named_scope(f"wait_{which}"):
            pltpu.make_async_copy(part, part, recv_sem.at[which]).wait()

    def sent(which, slots, count):
        part = slots.at[pl.ds(0, count)]
        pltpu.make_async_copy(part, part, send_sem.at[which]).wait()

    barrier = pltpu.get_barrier_semaphore()
    for device, _ in z_peers():
        pl.semaphore_signal(barrier, inc=1, device_id=device, device_id_type=MESH)
    for device, _ in plane_peers():
        pl.semaphore_signal(barrier, inc=1, device_id=device, device_id_type=MESH)

    eye = lax.broadcasted_iota(jnp.int32, (128, 128), 0) == lax.broadcasted_iota(
        jnp.int32, (128, 128), 1
    )
    diagonal = jnp.where(eye, 1.0, 0.0).astype(F32)
    with jax.named_scope("wait_small"):
        for copy in loads[:7]:
            copy.wait()

    lane = lax.broadcasted_iota(jnp.int32, (1, 128), 1)
    at = jnp.full((1, 128), -1, jnp.int32)
    for r in range(BLOCKS):
        for s in range(SLOTS):
            t = cols[r, s]
            row = (t & 0x181) | ((t & 0xE) << 3) | ((t & 0x70) >> 3)
            row = jnp.where(s < cnt[r], row, PLANE * Z * 2)
            rowid[r * SLOTS + s] = row
            at = jnp.where(lane == r * LANES + s, row, at)
    onehot[...] = jnp.where(
        lax.broadcasted_iota(jnp.int32, (PLANE * Z * 2, 128), 0) == at, 1.0, 0.0
    ).astype(BF16)
    table[pl.ds(PLANE * Z * 2, 8), :] = jnp.zeros((8, 128), F32)
    contrib[...] = jnp.zeros_like(contrib)
    beta_u = u_in[...] * beta[...]
    for r in range(BLOCKS):
        acc_ref[r] = jnp.where(eye, -beta_u[r : r + 1, :], 0.0)
    vz[z] = v_in[...]
    gsend[:, 0:4, :] = gram(lb[...]).reshape(PLANE, 4, 128)
    gsend[:, 4:8, :] = gram(rb[...]).reshape(PLANE, 4, 128)

    with jax.named_scope("wait_barrier"):
        pl.semaphore_wait(barrier, PLANE - 1 + Z - 1)

    for device, _ in z_peers():
        send(AG_Z, v_in, vz.at[z], device)
    for device, peer in plane_peers():
        send(G_P, gsend.at[peer], g_p.at[g], device)
    g_p[g] = gsend[g]
    arrived(AG_Z, vz, Z - 1)
    vtab[g] = vz[...].reshape(2 * Z, 128).astype(BF16)
    for device, _ in plane_peers():
        send(AG_P, vtab.at[g], vtab.at[g], device)
    arrived(G_P, g_p, PLANE - 1)
    gz = jnp.sum(g_p[...], axis=0)
    gz_send[...] = gz
    g_z[z] = gz
    for device, _ in z_peers():
        send(G_Z, gz_send, g_z.at[z], device)
    with jax.named_scope("wait_tiles"):
        for copy in loads[7:]:
            copy.wait()
    arrived(AG_P, vtab, PLANE - 1)
    table[pl.ds(0, PLANE * Z * 2), :] = vtab[...].astype(F32).reshape(PLANE * Z * 2, 128)

    ps = []
    for r in range(BLOCKS):

        def forward(s, acc, r=r):
            row = table[pl.ds(rowid[r * SLOTS + s], 1), :]
            return acc + tiles[r, s].astype(F32) * row

        acc = lax.fori_loop(0, SLOTS, forward, acc_ref[r], unroll=4)
        ps.append(jnp.broadcast_to(jnp.sum(acc, axis=1, keepdims=True), (128, 128)))

    def inner(basis_rows, columns):
        first = sum(
            jnp.sum(b * c, axis=0, keepdims=True) for b, c in zip(basis_rows, columns)
        )
        square = sum(jnp.sum(c * c, axis=0, keepdims=True) for c in columns)
        return first, square

    def total(slots):
        return jnp.sum(slots[...], axis=0)

    first, square = inner([lb[pl.ds(r * 128, 128), :] for r in range(BLOCKS)], ps)
    c_send[0:1, :] = first
    c_send[1:2, :] = square
    c_p[g] = c_send[...]
    for device, _ in plane_peers():
        send(C_P, c_send, c_p.at[g], device)
    for r in range(BLOCKS):
        acc_ref[r] = ps[r]
    arrived(G_Z, g_z, Z - 1)
    gp = jnp.sum(g_z[...], axis=0)
    gp_send[...] = gp
    g_all[g] = gp
    for device, _ in plane_peers():
        send(G_ALL, gp_send, g_all.at[g], device)
    arrived(C_P, c_p, PLANE - 1)
    cz = total(c_p)
    cz_send[...] = cz
    c_z[z] = cz
    for device, _ in z_peers():
        send(C_Z, cz_send, c_z.at[z], device)
    arrived(G_ALL, g_all, PLANE - 1)
    left_gram = g_all[:, 0:4, :].reshape(128, 128)
    right_gram = g_all[:, 4:8, :].reshape(128, 128)

    def twice(gram_matrix):
        b = 2.0 * diagonal - gram_matrix
        return b, 2.0 * b - high_dot(b, high_dot(gram_matrix, b))

    bl, nl[...] = twice(left_gram)
    ml[...] = high_dot(lb[...], bl)

    def norm_of(first, square, quadratic):
        column = jnp.sum(quadratic * first, axis=1, keepdims=True)
        inner_sum = jnp.sum(jnp.where(eye, column, 0.0) * first, axis=0, keepdims=True)
        inner_sum = jnp.sum(inner_sum, axis=1, keepdims=True)
        return jnp.sqrt(square - inner_sum + 1e-6)

    arrived(C_Z, c_z, Z - 1)
    both = total(c_z)
    first, square = both[0:1, :], both[1:2, :]
    alpha = norm_of(first, square, nl[...])
    contribs = []
    for r in range(BLOCKS):
        less = jnp.sum(ml[pl.ds(r * 128, 128), :] * first, axis=1, keepdims=True)
        u = (acc_ref[r] - less) / alpha
        u_ref[r] = u
        ub_ref[r] = u.astype(BF16).astype(F32)
    for r in range(BLOCKS):

        def backward(s, _, r=r):
            part = jnp.sum(tiles[r, s].astype(F32) * ub_ref[r], axis=0, keepdims=True)
            contrib[pl.ds(r * LANES + s, 1), :] = part
            return 0

        lax.fori_loop(0, SLOTS, backward, 0, unroll=4)
    whole = contrib[...]
    high = whole.astype(BF16)
    rest = whole - high.astype(F32)
    middle = rest.astype(BF16)
    low = (rest - middle.astype(F32)).astype(BF16)
    hot = onehot[...]
    partial = (
        jnp.dot(hot, high, preferred_element_type=F32)
        + jnp.dot(hot, middle, preferred_element_type=F32)
        + jnp.dot(hot, low, preferred_element_type=F32)
    )
    s_send[...] = partial.reshape(PLANE, 2 * Z, 128)
    for device, peer in plane_peers():
        send(S_P, s_send.at[peer], s_p.at[g], device)
    s_p[g] = s_send[g]
    for r in range(BLOCKS):
        out_ref[r : r + 1, :] = left_scale * jnp.sum(
            jnp.where(eye, u_ref[r], 0.0), axis=0, keepdims=True
        )
    br, nr[...] = twice(right_gram)
    mr[...] = high_dot(rb[...], br)
    arrived(S_P, s_p, PLANE - 1)
    sz_send[...] = total(s_p).reshape(Z, 2, 128)
    s_z[z] = sz_send[z]
    for device, peer in z_peers():
        send(S_Z, sz_send.at[peer], s_z.at[z], device)
    arrived(S_Z, s_z, Z - 1)
    residual = total(s_z) - alpha * v_in[...]
    rs = [
        jnp.broadcast_to(
            jnp.sum(jnp.where(eye, residual[h : h + 1, :], 0.0), axis=1, keepdims=True), (128, 128)
        )
        for h in range(2)
    ]
    first, square = inner([rb[pl.ds(h * 128, 128), :] for h in range(2)], rs)
    d_send[0:1, :] = first
    d_send[1:2, :] = square
    d_p[g] = d_send[...]
    for device, _ in plane_peers():
        send(D_P, d_send, d_p.at[g], device)
    arrived(D_P, d_p, PLANE - 1)
    dz = total(d_p)
    dz_send[...] = dz
    d_z[z] = dz
    for device, _ in z_peers():
        send(D_Z, dz_send, d_z.at[z], device)
    arrived(D_Z, d_z, Z - 1)
    both = total(d_z)
    first, square = both[0:1, :], both[1:2, :]
    new_beta = norm_of(first, square, nr[...])
    for h in range(2):
        less = jnp.sum(mr[pl.ds(h * 128, 128), :] * first, axis=1, keepdims=True)
        v = (rs[h] - less) / new_beta
        out_ref[4 + h : 5 + h, :] = right_scale * jnp.sum(
            jnp.where(eye, v, 0.0), axis=0, keepdims=True
        )
    out_ref[6:7, :] = jnp.where(lane == 0, alpha, new_beta)
    out_ref[7:8, :] = jnp.zeros((1, 128), F32)

    for which, slots, count in (
        (AG_Z, vz, Z - 1),
        (AG_P, vtab, PLANE - 1),
        (G_P, g_p, PLANE - 1),
        (G_Z, g_z, Z - 1),
        (G_ALL, g_all, PLANE - 1),
        (C_P, c_p, PLANE - 1),
        (C_Z, c_z, Z - 1),
        (S_P, s_p, PLANE - 1),
        (S_Z, s_z, Z - 1),
        (D_P, d_p, PLANE - 1),
        (D_Z, d_z, Z - 1),
    ):
        sent(which, slots, count)


def finish(out, left, right, coefs):
    left[...] = out[0:BLOCKS, :]
    right[...] = out[BLOCKS : BLOCKS + 2, :]
    coefs[0] = out[6, 0]
    coefs[1] = out[6, 1]


def solution(mesh):
    devices = math.prod(mesh.shape.values())

    def step(tiles, tile_cols, tile_count, u_start, v_start, beta_start, left_basis, right_basis):
        vmem = pltpu.VMEM
        out = pl.pallas_call(
            lambda *refs: kernel(
                math.sqrt(u_start.shape[0] * devices), math.sqrt(v_start.shape[0] * devices), *refs
            ),
            name="lanczos_step",
            out_shape=pltpu.VMEM((8, 128), F32),
            in_specs=[pl.BlockSpec(memory_space=pltpu.HBM)] * 8,
            out_specs=pl.BlockSpec(memory_space=pltpu.VMEM),
            scratch_shapes=[
                vmem((BLOCKS, SLOTS, 128, 128), BF16),
                pltpu.SMEM((BLOCKS, SLOTS), jnp.int32),
                pltpu.SMEM((BLOCKS,), jnp.int32),
                vmem((1, 1), F32),
                vmem((BLOCKS, 128), F32),
                vmem((2, 128), F32),
                vmem((BLOCKS * 128, 128), F32),
                vmem((2 * 128, 128), F32),
                pltpu.SMEM((BLOCKS * SLOTS,), jnp.int32),
                vmem((PLANE * Z * 2, 128), BF16),
                vmem((Z, 2, 128), F32),
                vmem((PLANE, 2 * Z, 128), BF16),
                vmem((PLANE * Z * 2 + 8, 128), F32),
                vmem((BLOCKS, 128, 128), F32),
                vmem((PLANE, 8, 128), F32),
                vmem((PLANE, 8, 128), F32),
                vmem((8, 128), F32),
                vmem((Z, 8, 128), F32),
                vmem((8, 128), F32),
                vmem((PLANE, 8, 128), F32),
                vmem((BLOCKS * 128, 128), F32),
                vmem((128, 128), F32),
                vmem((2 * 128, 128), F32),
                vmem((128, 128), F32),
                vmem((2, 128), F32),
                vmem((PLANE, 2, 128), F32),
                vmem((2, 128), F32),
                vmem((Z, 2, 128), F32),
                vmem((128, 128), F32),
                vmem((BLOCKS, 128, 128), F32),
                vmem((BLOCKS, 128, 128), F32),
                vmem((PLANE, 2 * Z, 128), F32),
                vmem((PLANE, 2 * Z, 128), F32),
                vmem((Z, 2, 128), F32),
                vmem((Z, 2, 128), F32),
                vmem((2, 128), F32),
                vmem((PLANE, 2, 128), F32),
                vmem((2, 128), F32),
                vmem((Z, 2, 128), F32),
                pltpu.SemaphoreType.DMA((7 + BLOCKS,)),
                pltpu.SemaphoreType.DMA((EXCHANGES,)),
                pltpu.SemaphoreType.DMA((EXCHANGES,)),
            ],
            compiler_params=pltpu.CompilerParams(
                collective_id=0, has_side_effects=True
            ),
        )(
            tiles,
            tile_cols,
            tile_count,
            u_start.reshape(BLOCKS, 128),
            v_start.reshape(2, 128),
            beta_start.reshape(1, 1),
            left_basis,
            right_basis,
        )
        left, right, coefs = pl.pallas_call(
            finish,
            name="finish",
            out_shape=(
                jax.ShapeDtypeStruct((BLOCKS, 128), F32),
                jax.ShapeDtypeStruct((2, 128), F32),
                jax.ShapeDtypeStruct((2,), F32),
            ),
            in_specs=[pl.BlockSpec(memory_space=pltpu.VMEM)],
            out_specs=(
                pl.BlockSpec(memory_space=pltpu.VMEM),
                pl.BlockSpec(memory_space=pltpu.VMEM),
                pl.BlockSpec(memory_space=pltpu.SMEM),
            ),
            compiler_params=pltpu.CompilerParams(vmem_limit_bytes=1 << 20),
        )(out)
        return left.reshape(1, -1), right.reshape(1, -1), coefs

    both = ("blk", "plane")
    return jax.shard_map(
        step,
        mesh=mesh,
        in_specs=(
            P(both, None, None, None),
            P(both, None),
            P(both),
            P(both),
            P(both),
            P(),
            P(both, None),
            P(both, None),
        ),
        out_specs=(P(None, both), P(None, both), P()),
        check_vma=False,
    )
```
